8 devices in a mesh: pp: 4 (over z, y, x), ep: 2 (over core).
Axes of the slice: x: 2, y: 2, z: 1, core: 2. Of those that a mesh axis runs over, the one named last changes fastest.
Arguments:
- expert_out: bfloat16 [8, 128, 48, 4096], P('pp', 'ep')
- expert_ids: int32 [8, 4, 128, 8], P('pp', 'ep')
- slot_ids: int32 [8, 4, 128, 8], P('pp', 'ep')
- gate_vals: float32 [8, 4, 128, 8], P('pp', 'ep')
- residual: bfloat16 [8, 4, 128, 4096], P('pp', 'ep')
- norm_w: float32 [4, 4096], P('pp')
- w_query: bfloat16 [4, 4096, 64, 128], P('pp')
- w_key: bfloat16 [4, 4096, 64, 128], P('pp')
- w_value: bfloat16 [4, 4096, 64, 128], P('pp')
- w_out: bfloat16 [4, 64, 128, 4096], P('pp')
Outputs:
- output: bfloat16 [8, 4, 128, 4096], P('pp', 'ep')
All inputs are finite; a program needn't handle non-finite values.
Results may differ from the reference program's by a relative error of at most 0.0139631.
Values are sent between devices in bfloat16 or wider.
A program may use at most 1.25 GiB of HBM per device.

```python
import jax
import jax.numpy as jnp
from jax import lax

STAGES = 4
GROUP_SIZE = 2
NUM_MICRO = 2
SEQ_LEN = 128
SEQS_PER_DEV = 2
D_MODEL = 4096
NUM_EXPERTS = 128
TOP_K = 8
NUM_HEADS = 64
HEAD_DIM = 128
SRC_SLOTS = 24

TOKENS_DEV = SEQS_PER_DEV * SEQ_LEN
SEQS_ALL = GROUP_SIZE * SEQS_PER_DEV
CAPACITY = GROUP_SIZE * SRC_SLOTS
NUM_ROWS = STAGES * NUM_MICRO
QKV_WIDTH = NUM_HEADS * HEAD_DIM
NORM_EPS = 1e-6


def block_ranks(block_ids):
    perm_order = jnp.argsort(block_ids, stable=True)
    sorted_ids = block_ids[perm_order]
    group_start = jnp.searchsorted(sorted_ids, sorted_ids, side='left')
    rank_sorted = jnp.arange(block_ids.shape[0]) - group_start
    return jnp.zeros_like(block_ids).at[perm_order].set(rank_sorted)


def draw_routing(route_key):
    key_bias, key_hot, key_shift, key_noise, key_order = jax.random.split(route_key, 5)
    expert_bias = jnp.sum(jax.random.randint(key_bias, (NUM_ROWS, NUM_EXPERTS, 4), 0, 166, jnp.int32), axis=-1)
    hot_expert = jax.random.randint(key_hot, (NUM_ROWS,), 0, NUM_EXPERTS)
    cover_shift = jax.random.randint(key_shift, (NUM_ROWS,), 0, NUM_EXPERTS)
    local_pos = jnp.arange(TOKENS_DEV)
    expert_pos = jnp.arange(NUM_EXPERTS)
    tie_break = (NUM_EXPERTS - 1 - expert_pos).astype(jnp.int32)

    def one_block(flat_idx):
        row_idx = flat_idx // GROUP_SIZE
        blk_idx = flat_idx % GROUP_SIZE
        noise_draws = jnp.sum(jax.random.randint(jax.random.fold_in(key_noise, flat_idx), (TOKENS_DEV, NUM_EXPERTS, 3), 0, 164, jnp.int32), axis=-1)
        token_pos = blk_idx * TOKENS_DEV + local_pos
        is_cover = (token_pos[:, None] + cover_shift[row_idx]) % NUM_EXPERTS == expert_pos[None, :]
        is_hot = expert_pos[None, :] == hot_expert[row_idx]
        score_int = (expert_bias[row_idx][None, :] + noise_draws) * NUM_EXPERTS + tie_break[None, :] + (1 << 22) * is_cover.astype(jnp.int32) + (1 << 23) * is_hot.astype(jnp.int32)
        chosen = lax.top_k(score_int, TOP_K)[1]
        order_bits = jax.random.bits(jax.random.fold_in(key_order, flat_idx), (TOKENS_DEV, TOP_K), jnp.uint32) >> 8
        order_key = order_bits * TOP_K + jnp.arange(TOP_K, dtype=jnp.uint32)[None, :]
        perm_order = jnp.argsort(order_key, axis=1)
        chosen = jnp.take_along_axis(chosen, perm_order, axis=1)
        slot_rank = block_ranks(chosen.reshape(TOKENS_DEV * TOP_K)).reshape(TOKENS_DEV, TOP_K)
        slot_ids = jnp.where(slot_rank < SRC_SLOTS, blk_idx * SRC_SLOTS + slot_rank, -1)
        return chosen.astype(jnp.int32), slot_ids.astype(jnp.int32)

    expert_ids, slot_ids = lax.map(one_block, jnp.arange(NUM_ROWS * GROUP_SIZE))
    route_shape = (NUM_ROWS, SEQS_ALL, SEQ_LEN, TOP_K)
    return expert_ids.reshape(route_shape), slot_ids.reshape(route_shape)


def draw_bf16(draw_key, arr_shape, scale_fac):
    def one_slice(slice_key):
        return (scale_fac * jax.random.normal(slice_key, arr_shape[1:], jnp.float32)).astype(jnp.bfloat16)
    return lax.map(one_slice, jax.random.split(draw_key, arr_shape[0]))


def setup_inputs(seed: int = 0) -> dict:
    root_key = jax.random.key(seed)
    sub_keys = jax.random.split(root_key, 10)
    expert_ids, slot_ids = draw_routing(sub_keys[0])
    gate_vals = jax.nn.softmax(1.5 * jax.random.normal(sub_keys[1], (NUM_ROWS, SEQS_ALL, SEQ_LEN, TOP_K), jnp.float32), axis=-1)
    expert_scale = 1.5 * jnp.exp(0.5 * jax.random.normal(sub_keys[2], (NUM_ROWS * NUM_EXPERTS,), jnp.float32))

    def expert_slab(slab_args):
        slab_key, slab_scale = slab_args
        return (slab_scale * jax.random.normal(slab_key, (CAPACITY, D_MODEL), jnp.float32)).astype(jnp.bfloat16)

    expert_out = lax.map(expert_slab, (jax.random.split(sub_keys[3], NUM_ROWS * NUM_EXPERTS), expert_scale))
    expert_out = expert_out.reshape(NUM_ROWS, NUM_EXPERTS, CAPACITY, D_MODEL)
    residual = draw_bf16(sub_keys[4], (NUM_ROWS * SEQS_ALL, SEQ_LEN, D_MODEL), 1.0)
    residual = residual.reshape(NUM_ROWS, SEQS_ALL, SEQ_LEN, D_MODEL)
    norm_w = 1.0 + 0.4 * jax.random.normal(sub_keys[5], (STAGES, D_MODEL), jnp.float32)
    in_scale = D_MODEL ** -0.5
    out_scale = QKV_WIDTH ** -0.5
    w_query = draw_bf16(sub_keys[6], (STAGES, D_MODEL, NUM_HEADS, HEAD_DIM), 1.5 * in_scale)
    w_key = draw_bf16(sub_keys[7], (STAGES, D_MODEL, NUM_HEADS, HEAD_DIM), 1.5 * in_scale)
    w_value = draw_bf16(sub_keys[8], (STAGES, D_MODEL, NUM_HEADS, HEAD_DIM), in_scale)
    w_out = draw_bf16(sub_keys[9], (STAGES, NUM_HEADS, HEAD_DIM, D_MODEL), out_scale)
    return dict(expert_out=expert_out, expert_ids=expert_ids, slot_ids=slot_ids, gate_vals=gate_vals, residual=residual, norm_w=norm_w, w_query=w_query, w_key=w_key, w_value=w_value, w_out=w_out)


def reference(expert_out, expert_ids, slot_ids, gate_vals, residual, norm_w, w_query, w_key, w_value, w_out):
    causal = jnp.arange(SEQ_LEN)[:, None] >= jnp.arange(SEQ_LEN)[None, :]

    def one_stage(stage_idx):
        src_stage = (stage_idx + STAGES - 1) % STAGES
        stage_norm = norm_w[stage_idx]
        stage_wq = w_query[stage_idx].reshape(D_MODEL, QKV_WIDTH)
        stage_wk = w_key[stage_idx].reshape(D_MODEL, QKV_WIDTH)
        stage_wv = w_value[stage_idx].reshape(D_MODEL, QKV_WIDTH)
        stage_wo = w_out[stage_idx].reshape(QKV_WIDTH, D_MODEL)

        def project(x_in, weight_mat):
            head_out = jnp.dot(x_in, weight_mat, preferred_element_type=jnp.float32).astype(jnp.bfloat16)
            return head_out.reshape(SEQ_LEN, NUM_HEADS, HEAD_DIM).astype(jnp.float32)

        def one_sequence(flat_idx):
            src_row = src_stage * NUM_MICRO + flat_idx // SEQS_ALL
            seq_idx = flat_idx % SEQS_ALL
            ids_seq = expert_ids[src_row, seq_idx]
            slot_seq = slot_ids[src_row, seq_idx]
            is_kept = slot_seq >= 0
            picked = expert_out[src_row, ids_seq, jnp.where(is_kept, slot_seq, 0)].astype(jnp.float32)
            weight = jnp.where(is_kept, gate_vals[src_row, seq_idx], 0.0)
            mixed_sum = residual[src_row, seq_idx].astype(jnp.float32) + jnp.sum(weight[:, :, None] * picked, axis=1)
            y_wide = mixed_sum.astype(jnp.bfloat16).astype(jnp.float32)
            inv_rms = lax.rsqrt(jnp.mean(y_wide * y_wide, axis=-1, keepdims=True) + NORM_EPS)
            x_in = (y_wide * inv_rms * stage_norm).astype(jnp.bfloat16)
            q_heads = project(x_in, stage_wq)
            k_heads = project(x_in, stage_wk)
            v_heads = project(x_in, stage_wv)
            scores = jnp.einsum('qhe,khe->hqk', q_heads, k_heads) * HEAD_DIM ** -0.5
            attn_probs = jax.nn.softmax(jnp.where(causal, scores, -jnp.inf), axis=-1).astype(jnp.bfloat16)
            attn_out = jnp.einsum('hqk,khe->qhe', attn_probs.astype(jnp.float32), v_heads).astype(jnp.bfloat16)
            out_proj = jnp.dot(attn_out.reshape(SEQ_LEN, QKV_WIDTH), stage_wo, preferred_element_type=jnp.float32).astype(jnp.bfloat16)
            return (y_wide + out_proj.astype(jnp.float32)).astype(jnp.bfloat16)

        return lax.map(one_sequence, jnp.arange(NUM_MICRO * SEQS_ALL))

    stage_outs = lax.map(one_stage, jnp.arange(STAGES))
    return stage_outs.reshape(NUM_ROWS, SEQS_ALL, SEQ_LEN, D_MODEL)
```

```python
import functools

import jax
import jax.numpy as jnp
from jax import lax
from jax.experimental import pallas as pl
from jax.experimental.pallas import tpu as pltpu
from jax.sharding import PartitionSpec as P


NORM_EPS = 1e-6
COL = 512


def split_gate(full):
    hi = full.astype(jnp.bfloat16)
    rest = full - hi.astype(jnp.float32)
    mid = rest.astype(jnp.bfloat16)
    lo = (rest - mid.astype(jnp.float32)).astype(jnp.bfloat16)
    return hi, mid, lo


def mix_kernel(has_add, side_ref, code_ref, gate_ref, exp_ref, *rest):
    if has_add:
        res_ref, part_ref, out_ref, w_ref = rest
    else:
        out_ref, w_ref = rest
    tokens, top_k = code_ref.shape
    slots = w_ref.shape[2]

    @pl.when(pl.program_id(0) == 0)
    def build():
        for t0 in range(0, tokens, 64):
            code = code_ref[t0:t0 + 64, :]
            gate = gate_ref[t0:t0 + 64, :]
            for s0 in range(0, slots, 512):
                lane = lax.broadcasted_iota(jnp.int32, (64, 512), 1) + s0
                full = jnp.zeros((64, 512), jnp.float32)
                for i in range(top_k):
                    full = jnp.where(lane == code[:, i:i + 1], gate[:, i:i + 1], full)
                for part, val in enumerate(split_gate(full)):
                    w_ref[part, t0:t0 + 64, s0:s0 + 512] = val

    exp_rows = exp_ref[0].reshape(slots, exp_ref.shape[3])
    total = jnp.dot(w_ref[0], exp_rows, preferred_element_type=jnp.float32)
    total += jnp.dot(w_ref[1], exp_rows, preferred_element_type=jnp.float32)
    total += jnp.dot(w_ref[2], exp_rows, preferred_element_type=jnp.float32)
    if has_add:
        total = total + part_ref[...] + res_ref[...].astype(jnp.float32)
    out_ref[...] = total.astype(out_ref.dtype)


def mix(expert_out, row, side, code, gate, add=None):
    tokens, top_k = code.shape
    _, experts, cap, d_model = expert_out.shape
    half = cap // 2
    small = pl.BlockSpec((tokens, top_k), lambda c, s: (0, 0))
    cols = pl.BlockSpec((tokens, COL), lambda c, s: (0, c))
    in_specs = [small, small, pl.BlockSpec((1, experts, half, COL), lambda c, s: (row, 0, s[0], c))]
    args = [code, gate, expert_out]
    if add is not None:
        in_specs += [cols, cols]
        args += list(add)
    slots = experts * half
    return pl.pallas_call(
        functools.partial(mix_kernel, add is not None),
        out_shape=jax.ShapeDtypeStruct((tokens, d_model), jnp.float32 if add is None else jnp.bfloat16),
        grid_spec=pltpu.PrefetchScalarGridSpec(
            num_scalar_prefetch=1,
            grid=(d_model // COL,),
            in_specs=in_specs,
            out_specs=cols,
            scratch_shapes=[pltpu.VMEM((3, tokens, slots), jnp.bfloat16)],
        ),
        cost_estimate=pl.CostEstimate(flops=6 * tokens * slots * d_model, bytes_accessed=2 * slots * d_model, transcendentals=0),
    )(side.reshape(1), *args)


def attn_kernel(seq_len, q_ref, k_ref, v_ref, o_ref):
    heads, tokens, head_dim = q_ref.shape
    row = lax.broadcasted_iota(jnp.int32, (seq_len, seq_len), 0)
    col = lax.broadcasted_iota(jnp.int32, (seq_len, seq_len), 1)
    causal = row >= col
    for h in range(heads):
        for t0 in range(0, tokens, seq_len):
            q = q_ref[h, t0:t0 + seq_len, :]
            k = k_ref[h, t0:t0 + seq_len, :]
            v = v_ref[h, t0:t0 + seq_len, :]
            scores = lax.dot_general(q, k, (((1,), (1,)), ((), ())), preferred_element_type=jnp.float32) * (head_dim ** -0.5)
            scores = jnp.where(causal, scores, -jnp.inf)
            expd = jnp.exp(scores - jnp.max(scores, axis=1, keepdims=True))
            probs = (expd / jnp.sum(expd, axis=1, keepdims=True)).astype(jnp.bfloat16)
            out = jnp.dot(probs, v, preferred_element_type=jnp.float32).astype(jnp.bfloat16)
            o_ref[t0:t0 + seq_len, h * head_dim:(h + 1) * head_dim] = out


def attention(q, k, v, seq_len):
    heads, tokens, head_dim = q.shape
    group = 8
    spec = pl.BlockSpec((group, tokens, head_dim), lambda g: (g, 0, 0))
    return pl.pallas_call(
        functools.partial(attn_kernel, seq_len),
        out_shape=jax.ShapeDtypeStruct((tokens, heads * head_dim), jnp.bfloat16),
        grid=(heads // group,),
        in_specs=[spec] * 3,
        out_specs=pl.BlockSpec((tokens, group * head_dim), lambda g: (0, g)),
        cost_estimate=pl.CostEstimate(flops=16 * tokens * seq_len * heads * head_dim, bytes_accessed=8 * tokens * heads * head_dim, transcendentals=tokens * seq_len * heads),
    )(q, k, v)


def attention_block(combined, seq_len, norm_w, w_query, w_key, w_value, w_out):
    y_wide = combined.astype(jnp.float32)
    inv_rms = lax.rsqrt(jnp.mean(y_wide * y_wide, axis=-1, keepdims=True) + NORM_EPS)
    x_in = (y_wide * inv_rms * norm_w).astype(jnp.bfloat16)
    heads = []
    for w in (w_query, w_key, w_value):
        heads.append(jnp.einsum('td,dhe->hte', x_in, w, preferred_element_type=jnp.float32).astype(jnp.bfloat16))
    attn_out = attention(*heads, seq_len)
    w_flat = w_out.reshape(-1, w_out.shape[-1])
    out_proj = jnp.dot(attn_out, w_flat, preferred_element_type=jnp.float32).astype(jnp.bfloat16)
    return (y_wide + out_proj.astype(jnp.float32)).astype(jnp.bfloat16)


def solution(mesh):
    stages = mesh.shape['pp']
    send_next = [(src_row, (src_row + 1) % stages) for src_row in range(stages)]
    swap = [(0, 1), (1, 0)]
    tok_spec = P('pp', 'ep', None, None)
    wt_spec = P('pp', None, None, None)

    def step(expert_out, expert_ids, slot_ids, gate_vals, residual, norm_w, w_query, w_key, w_value, w_out):
        num_micro, seqs_dev, seq_len, d_model = residual.shape
        experts, cap = expert_out.shape[1:3]
        half = cap // 2
        tokens = seqs_dev * seq_len
        me = lax.axis_index('ep').astype(jnp.int32)
        code = jnp.where(slot_ids >= 0, expert_ids * half + slot_ids - me * half, -1)
        theirs = lax.ppermute(jnp.stack([code.astype(jnp.float32), gate_vals]), 'ep', swap)
        code = code.reshape(num_micro, tokens, -1)
        gate = gate_vals.reshape(num_micro, tokens, -1)
        their_code = theirs[0].astype(jnp.int32).reshape(num_micro, tokens, -1)
        their_gate = theirs[1].reshape(num_micro, tokens, -1)
        first = me * experts * half
        flat_h = residual.reshape(num_micro, tokens, d_model)
        arrived = []
        for m in range(num_micro):
            part = mix(expert_out, m, 1 - me, their_code[m] - first, their_gate[m])
            got = lax.ppermute(part, 'ep', swap)
            y = mix(expert_out, m, me, code[m] - first, gate[m], (flat_h[m], got))
            arrived.append(lax.ppermute(y, 'pp', send_next))
        outs = [attention_block(y, seq_len, norm_w[0], w_query[0], w_key[0], w_value[0], w_out[0]) for y in arrived]
        return jnp.stack(outs).reshape(num_micro, seqs_dev, seq_len, d_model)

    return jax.shard_map(step, mesh=mesh, in_specs=(tok_spec, tok_spec, tok_spec, tok_spec, tok_spec, P('pp', None), wt_spec, wt_spec, wt_spec, wt_spec), out_specs=tok_spec, check_vma=False)
```

```python
import functools

import jax
import jax.numpy as jnp
from jax import lax
from jax.experimental import pallas as pl
from jax.experimental.pallas import tpu as pltpu
from jax.sharding import PartitionSpec as P


NORM_EPS = 1e-6
GROUP = 8
HALVES = 2


def gates_kernel(code_ref, gate_ref, after_ref, w_ref):
    tokens, top_k = code_ref.shape[1:]
    slots = w_ref.shape[2]
    rows, lanes = 64, 512
    for t0 in range(0, tokens, rows):
        code = code_ref[0, t0:t0 + rows, :]
        gate = gate_ref[0, t0:t0 + rows, :]
        for s0 in range(0, slots, lanes):
            lane = lax.broadcasted_iota(jnp.int32, (rows, lanes), 1) + s0
            full = jnp.zeros((rows, lanes), jnp.float32)
            for i in range(top_k):
                full = jnp.where(lane == code[:, i:i + 1], gate[:, i:i + 1], full)
            for part in range(3):
                val = full.astype(jnp.bfloat16)
                w_ref[0, part * tokens + t0:part * tokens + t0 + rows, s0:s0 + lanes] = val
                full = full - val.astype(jnp.float32)


def gates(code, gate, slots, after):
    rows, tokens, top_k = code.shape
    spec = pl.BlockSpec((1, tokens, top_k), lambda m: (m, 0, 0))
    return pl.pallas_call(
        gates_kernel,
        out_shape=jax.ShapeDtypeStruct((rows, 3 * tokens, slots), jnp.bfloat16),
        grid=(rows,),
        in_specs=[spec, spec, pl.BlockSpec(memory_space=pl.ANY)],
        out_specs=pl.BlockSpec((1, 3 * tokens, slots), lambda m: (m, 0, 0)),
        cost_estimate=pl.CostEstimate(flops=rows * tokens * slots * 64, bytes_accessed=6 * rows * tokens * slots, transcendentals=0),
        name='gates',
    )(code, gate, after)


def mix_kernel(has_add, side_ref, w_ref, exp_ref, after_ref, *rest):
    out_ref = rest[2] if has_add else rest[0]
    slots = w_ref.shape[2]
    tokens = w_ref.shape[1] // 3
    exp_rows = exp_ref[0].reshape(slots, exp_ref.shape[3])
    parts = jnp.dot(w_ref[0], exp_rows, preferred_element_type=jnp.float32)
    total = parts[:tokens] + parts[tokens:2 * tokens] + parts[2 * tokens:]
    if has_add:
        total = total + rest[1][...] + rest[0][...].astype(jnp.float32)
    out_ref[...] = total.astype(out_ref.dtype)
    if has_add:
        square_ref = rest[3]

        @pl.when(pl.program_id(0) == 0)
        def clear():
            square_ref[...] = jnp.zeros_like(square_ref)

        wide = total.astype(jnp.bfloat16).astype(jnp.float32)
        square_ref[...] += jnp.sum(wide * wide, axis=1, keepdims=True)


def mix(expert_out, row, piece, side, w, after, add=None):
    _, rows3, slots = w.shape
    tokens = rows3 // 3
    _, experts, cap, d_model = expert_out.shape
    width = d_model // HALVES
    col = 512
    steps = width // col
    in_specs = [
        pl.BlockSpec((1, rows3, slots), lambda c, s: (row, 0, 0)),
        pl.BlockSpec((1, experts, cap // 2, col), lambda c, s: (row, 0, s[0], piece * steps + c)),
        pl.BlockSpec(memory_space=pl.ANY),
    ]
    args = [w, expert_out, after]
    if add is not None:
        in_specs += [
            pl.BlockSpec((tokens, col), lambda c, s: (row, piece * steps + c)),
            pl.BlockSpec((tokens, col), lambda c, s: (0, c)),
        ]
        args += list(add)
    out_shape = [jax.ShapeDtypeStruct((tokens, width), jnp.float32 if add is None else jnp.bfloat16)]
    out_specs = [pl.BlockSpec((tokens, col), lambda c, s: (0, c))]
    if add is not None:
        out_shape.append(jax.ShapeDtypeStruct((tokens, 128), jnp.float32))
        out_specs.append(pl.BlockSpec((tokens, 128), lambda c, s: (0, 0)))
    return pl.pallas_call(
        functools.partial(mix_kernel, add is not None),
        out_shape=out_shape,
        grid_spec=pltpu.PrefetchScalarGridSpec(
            num_scalar_prefetch=1,
            grid=(steps,),
            in_specs=in_specs,
            out_specs=out_specs,
        ),
        cost_estimate=pl.CostEstimate(flops=2 * rows3 * slots * width, bytes_accessed=2 * slots * width, transcendentals=0),
    )(side.reshape(1), *args)


def normed(y_refs, inv_ref, norm_ref, xs):
    step = pl.program_id(1)

    @pl.when(pl.program_id(0) == 0)
    def make():
        rows = y_refs[0].shape[0]
        for m, y_ref in enumerate(y_refs):
            for t0 in range(0, rows, 64):
                span = slice(m * rows + t0, m * rows + t0 + 64)
                wide = y_ref[t0:t0 + 64, :].astype(jnp.float32)
                xs[step, span, :] = (wide * inv_ref[span, :1] * norm_ref[...]).astype(jnp.bfloat16)

    return xs[step]


def first_kernel(y0_ref, y1_ref, inv_ref, norm_ref, *refs):
    step = pl.program_id(1)
    x = normed((y0_ref, y1_ref), inv_ref, norm_ref, refs[6])
    for w_ref, o_ref in zip(refs[:3], refs[3:6]):
        depth = w_ref.shape[0]
        out = jnp.dot(x, w_ref[...].reshape(depth, -1), preferred_element_type=jnp.float32)

        @pl.when(step == 0)
        def start(out=out, o_ref=o_ref):
            o_ref[...] = out

        @pl.when(step > 0)
        def add(out=out, o_ref=o_ref):
            o_ref[...] += out


def attend(causal, scale, q, k, v):
    dims = (((1,), (1,)), ((), ()))
    scores = [lax.dot_general(a, b, dims, preferred_element_type=jnp.float32) for a, b in zip(q, k)]
    scores = [jnp.where(causal, s * scale, -jnp.inf) for s in scores]
    tops = [jnp.max(s, axis=1, keepdims=True) for s in scores]
    expd = [jnp.exp(s - t) for s, t in zip(scores, tops)]
    inv = [1.0 / jnp.sum(e, axis=1, keepdims=True) for e in expd]
    probs = [(e * i).astype(jnp.bfloat16) for e, i in zip(expd, inv)]
    return [jnp.dot(p, c, preferred_element_type=jnp.float32).astype(jnp.bfloat16) for p, c in zip(probs, v)]


def second_kernel(seq_len, head_dim, y0_ref, y1_ref, inv_ref, norm_ref, *refs):
    w_refs, p_refs, a_ref, accs, qkv = refs[:3], refs[3:6], refs[6], refs[7:10], refs[10]
    step = pl.program_id(1)
    last = pl.num_programs(1) - 1
    x = normed((y0_ref, y1_ref), inv_ref, norm_ref, refs[11])
    for i, w_ref in enumerate(w_refs):
        depth = w_ref.shape[0]
        out = jnp.dot(x, w_ref[...].reshape(depth, -1), preferred_element_type=jnp.float32)

        @pl.when(step == 0)
        def start(i=i, out=out):
            accs[i][...] = p_refs[i][...] + out

        @pl.when(step == last)
        def finish(i=i, out=out):
            qkv[i] = (accs[i][...] + out).astype(jnp.bfloat16)

    @pl.when(step == last)
    def heads():
        tokens, width = a_ref.shape
        row = lax.broadcasted_iota(jnp.int32, (seq_len, seq_len), 0)
        col = lax.broadcasted_iota(jnp.int32, (seq_len, seq_len), 1)
        causal = row >= col
        spans = [(t, h) for h in range(0, width, head_dim) for t in range(0, tokens, seq_len)]
        for n in range(0, len(spans), 8):
            part = spans[n:n + 8]
            args = [[qkv[i, t:t + seq_len, h:h + head_dim] for t, h in part] for i in range(3)]
            for (t, h), out in zip(part, attend(causal, head_dim ** -0.5, *args)):
                a_ref[t:t + seq_len, h:h + head_dim] = out


def project(piece, ys, inv, norm_w, weights, parts, seq_len):
    rows, width = ys[0].shape
    tokens = inv.shape[0]
    _, heads, head_dim = weights[0].shape
    depth = 1024
    steps = width // depth
    cols = GROUP * head_dim
    y_spec = pl.BlockSpec((rows, depth), lambda g, k: (0, jnp.where(g == 0, k, steps - 1)))
    w_spec = pl.BlockSpec((depth, GROUP, head_dim), lambda g, k: (piece * steps + k, g, 0))
    o_spec = pl.BlockSpec((tokens, cols), lambda g, k: (0, g))
    in_specs = [
        y_spec,
        y_spec,
        pl.BlockSpec(inv.shape, lambda g, k: (0, 0)),
        pl.BlockSpec((1, depth), lambda g, k: (0, piece * steps + k)),
    ] + [w_spec] * 3
    xs = pltpu.VMEM((steps, tokens, depth), jnp.bfloat16)
    flops = 6 * tokens * width * heads * head_dim
    settings = dict(
        grid=(heads // GROUP, steps),
        compiler_params=pltpu.CompilerParams(vmem_limit_bytes=56 * 2 ** 20),
        cost_estimate=pl.CostEstimate(flops=flops, bytes_accessed=flops // tokens, transcendentals=0),
    )
    args = (*ys, inv, norm_w, *weights)
    if parts is None:
        return pl.pallas_call(
            first_kernel,
            out_shape=[jax.ShapeDtypeStruct((tokens, heads * head_dim), jnp.float32)] * 3,
            in_specs=in_specs,
            out_specs=[o_spec] * 3,
            scratch_shapes=[xs],
            name='first',
            **settings,
        )(*args)
    assert steps == 2
    return pl.pallas_call(
        functools.partial(second_kernel, seq_len, head_dim),
        out_shape=jax.ShapeDtypeStruct((tokens, heads * head_dim), jnp.bfloat16),
        in_specs=in_specs + [o_spec] * 3,
        out_specs=o_spec,
        scratch_shapes=[pltpu.VMEM((tokens, cols), jnp.float32)] * 3 + [pltpu.VMEM((3, tokens, cols), jnp.bfloat16), xs],
        name='second',
        **settings,
    )(*args, *parts)


def out_kernel(y_refs_per_half, a_ref, w_ref, *refs):
    o_ref = refs[-1]
    out = jnp.dot(a_ref[...], w_ref[...], preferred_element_type=jnp.float32).astype(jnp.bfloat16).astype(jnp.float32)
    steps = pl.num_programs(0) // HALVES
    rows = refs[0].shape[0]
    for c in range(HALVES):

        @pl.when(pl.program_id(0) // steps == c)
        def store(c=c):
            for m in range(y_refs_per_half):
                wide = refs[c * y_refs_per_half + m][...].astype(jnp.float32)
                span = slice(m * rows, (m + 1) * rows)
                o_ref[span, :] = (wide + out[span]).astype(jnp.bfloat16)


def project_out(attn, w_out, ys):
    tokens, inner = attn.shape
    d_model = w_out.shape[1]
    col = 512
    steps = d_model // HALVES // col
    y_specs = [
        pl.BlockSpec((y.shape[0], col), lambda n, c=c: (0, jnp.clip(n - c * steps, 0, steps - 1)))
        for c in range(HALVES) for y in ys[c]
    ]
    flops = 2 * tokens * inner * d_model
    return pl.pallas_call(
        functools.partial(out_kernel, len(ys[0])),
        out_shape=jax.ShapeDtypeStruct((tokens, d_model), jnp.bfloat16),
        grid=(HALVES * steps,),
        in_specs=[pl.BlockSpec((tokens, inner), lambda n: (0, 0)), pl.BlockSpec((inner, col), lambda n: (0, n))] + y_specs,
        out_specs=pl.BlockSpec((tokens, col), lambda n: (0, n)),
        compiler_params=pltpu.CompilerParams(vmem_limit_bytes=56 * 2 ** 20),
        cost_estimate=pl.CostEstimate(flops=flops, bytes_accessed=flops // tokens, transcendentals=0),
        name='out',
    )(attn, w_out, *ys[0], *ys[1])


def solution(mesh):
    stages = mesh.shape['pp']
    send_next = [(src_row, (src_row + 1) % stages) for src_row in range(stages)]
    swap = [(0, 1), (1, 0)]
    tok_spec = P('pp', 'ep', None, None)
    wt_spec = P('pp', None, None, None)

    def step(expert_out, expert_ids, slot_ids, gate_vals, residual, norm_w, w_query, w_key, w_value, w_out):
        num_micro, seqs_dev, seq_len, d_model = residual.shape
        experts, cap = expert_out.shape[1:3]
        half = cap // 2
        slots = experts * half
        tokens = seqs_dev * seq_len
        me = lax.axis_index('ep').astype(jnp.int32)
        code = jnp.where(slot_ids >= 0, expert_ids * half + slot_ids - me * half, -1)
        theirs = lax.ppermute(jnp.stack([code.astype(jnp.float32), gate_vals]), 'ep', swap)
        flat = (num_micro, tokens, -1)
        first = me * slots
        w_own = gates(code.reshape(flat) - first, gate_vals.reshape(flat), slots, norm_w)
        w_their = gates(theirs[0].astype(jnp.int32).reshape(flat) - first, theirs[1].reshape(flat), slots, w_own)
        flat_h = residual.reshape(num_micro * tokens, d_model)
        arrived, squares, after = [], 0.0, w_their
        for c in range(HALVES):
            got = []
            for m in range(num_micro):
                part, = mix(expert_out, m, c, 1 - me, w_their, after)
                got.append(lax.ppermute(part, 'ep', swap))
                after = part
            ys, sums = [], []
            for m in range(num_micro):
                after, total = mix(expert_out, m, c, me, w_own, after, (flat_h, got[m]))
                sums.append(total[:, 0])
                ys.append(lax.ppermute(after, 'pp', send_next))
            arrived.append(ys)
            squares += jnp.stack(sums)
        squares = lax.ppermute(squares, 'pp', send_next)
        inv_rms = lax.rsqrt(squares.reshape(-1, 1) / d_model + NORM_EPS)
        inv_rms = jnp.broadcast_to(inv_rms, (num_micro * tokens, 128))
        weights = (w_query[0], w_key[0], w_value[0])
        out = None
        for c in range(HALVES):
            out = project(c, arrived[c], inv_rms, norm_w, weights, out, seq_len)
        result = project_out(out, w_out[0].reshape(-1, d_model), arrived)
        return result.reshape(num_micro, seqs_dev, seq_len, d_model)

    return jax.shard_map(step, mesh=mesh, in_specs=(tok_spec, tok_spec, tok_spec, tok_spec, tok_spec, P('pp', None), wt_spec, wt_spec, wt_spec, wt_spec), out_specs=tok_spec, check_vma=False)
```

```python
import functools

import jax
import jax.numpy as jnp
from jax import lax
from jax.experimental import pallas as pl
from jax.experimental.pallas import tpu as pltpu
from jax.sharding import PartitionSpec as P


NORM_EPS = 1e-6
GROUP = 16
HALVES = 2


def gates_kernel(code_ref, gate_ref, after_ref, w_ref):
    tokens, top_k = code_ref.shape[1:]
    slots = w_ref.shape[2]
    rows, lanes = 64, 512
    for t0 in range(0, tokens, rows):
        code = code_ref[0, t0:t0 + rows, :]
        gate = gate_ref[0, t0:t0 + rows, :]
        for s0 in range(0, slots, lanes):
            lane = lax.broadcasted_iota(jnp.int32, (rows, lanes), 1) + s0
            full = jnp.zeros((rows, lanes), jnp.float32)
            for i in range(top_k):
                full = jnp.where(lane == code[:, i:i + 1], gate[:, i:i + 1], full)
            for part in range(3):
                val = full.astype(jnp.bfloat16)
                w_ref[0, part * tokens + t0:part * tokens + t0 + rows, s0:s0 + lanes] = val
                full = full - val.astype(jnp.float32)


def gates(code, gate, slots, after):
    rows, tokens, top_k = code.shape
    spec = pl.BlockSpec((1, tokens, top_k), lambda m: (m, 0, 0))
    return pl.pallas_call(
        gates_kernel,
        out_shape=jax.ShapeDtypeStruct((rows, 3 * tokens, slots), jnp.bfloat16),
        grid=(rows,),
        in_specs=[spec, spec, pl.BlockSpec(memory_space=pl.ANY)],
        out_specs=pl.BlockSpec((1, 3 * tokens, slots), lambda m: (m, 0, 0)),
        compiler_params=pltpu.CompilerParams(vmem_limit_bytes=16 * 2 ** 20),
        cost_estimate=pl.CostEstimate(flops=rows * tokens * slots * 64, bytes_accessed=6 * rows * tokens * slots, transcendentals=0),
        name='gates',
    )(code, gate, after)


def mix_kernel(has_add, side_ref, w_ref, exp_ref, after_ref, *rest):
    out_ref = rest[2] if has_add else rest[0]
    slots = w_ref.shape[2]
    tokens = w_ref.shape[1] // 3
    exp_rows = exp_ref[0].reshape(slots, exp_ref.shape[3])
    parts = jnp.dot(w_ref[0], exp_rows, preferred_element_type=jnp.float32)
    total = parts[:tokens] + parts[tokens:2 * tokens] + parts[2 * tokens:]
    if has_add:
        total = total + rest[1][...] + rest[0][...].astype(jnp.float32)
    out_ref[...] = total.astype(out_ref.dtype)
    if has_add:
        square_ref = rest[3]

        @pl.when(pl.program_id(0) == 0)
        def clear():
            square_ref[...] = jnp.zeros_like(square_ref)

        wide = total.astype(jnp.bfloat16).astype(jnp.float32)
        square_ref[...] += jnp.sum(wide * wide, axis=1, keepdims=True)


def mix(expert_out, row, piece, side, w, after, add=None):
    _, rows3, slots = w.shape
    tokens = rows3 // 3
    _, experts, cap, d_model = expert_out.shape
    width = d_model // HALVES
    col = 512
    steps = width // col
    in_specs = [
        pl.BlockSpec((1, rows3, slots), lambda c, s: (row, 0, 0)),
        pl.BlockSpec((1, experts, cap // 2, col), lambda c, s: (row, 0, s[0], piece * steps + c)),
        pl.BlockSpec(memory_space=pl.ANY),
    ]
    args = [w, expert_out, after]
    if add is not None:
        in_specs += [
            pl.BlockSpec((tokens, col), lambda c, s: (row, piece * steps + c)),
            pl.BlockSpec((tokens, col), lambda c, s: (0, c)),
        ]
        args += list(add)
    out_shape = [jax.ShapeDtypeStruct((tokens, width), jnp.float32 if add is None else jnp.bfloat16)]
    out_specs = [pl.BlockSpec((tokens, col), lambda c, s: (0, c))]
    if add is not None:
        out_shape.append(jax.ShapeDtypeStruct((tokens, 128), jnp.float32))
        out_specs.append(pl.BlockSpec((tokens, 128), lambda c, s: (0, 0)))
    return pl.pallas_call(
        functools.partial(mix_kernel, add is not None),
        out_shape=out_shape,
        grid_spec=pltpu.PrefetchScalarGridSpec(
            num_scalar_prefetch=1,
            grid=(steps,),
            in_specs=in_specs,
            out_specs=out_specs,
        ),
        compiler_params=pltpu.CompilerParams(vmem_limit_bytes=16 * 2 ** 20),
        cost_estimate=pl.CostEstimate(flops=2 * rows3 * slots * width, bytes_accessed=2 * slots * width, transcendentals=0),
    )(side.reshape(1), *args)


def normed(first_step, step, y_refs, inv_ref, norm_ref, xs):
    @pl.when(first_step)
    def make():
        rows = y_refs[0].shape[0]
        for m, y_ref in enumerate(y_refs):
            for t0 in range(0, rows, 64):
                span = slice(m * rows + t0, m * rows + t0 + 64)
                wide = y_ref[t0:t0 + 64, :].astype(jnp.float32)
                xs[step, span, :] = (wide * inv_ref[span, :1] * norm_ref[...]).astype(jnp.bfloat16)

    return xs[step]


def first_kernel(y0_ref, y1_ref, inv_ref, norm_ref, *refs):
    step = pl.program_id(1)
    o_ref = refs[3]
    x = normed(pl.program_id(0) == 0, step, (y0_ref, y1_ref), inv_ref, norm_ref, refs[4])
    for i, w_ref in enumerate(refs[:3]):
        depth = w_ref.shape[0]
        base = jnp.where(step == 0, 0.0, o_ref[i])
        o_ref[i] = base + jnp.dot(x, w_ref[...].reshape(depth, -1), preferred_element_type=jnp.float32)


def attend(causal, scale, q, k, v):
    dims = (((1,), (1,)), ((), ()))
    scores = [lax.dot_general(a, b, dims, preferred_element_type=jnp.float32) for a, b in zip(q, k)]
    scores = [jnp.where(causal, s * scale, -jnp.inf) for s in scores]
    tops = [jnp.max(s, axis=1, keepdims=True) for s in scores]
    expd = [jnp.exp(s - t) for s, t in zip(scores, tops)]
    inv = [1.0 / jnp.sum(e, axis=1, keepdims=True) for e in expd]
    probs = [(e * i).astype(jnp.bfloat16) for e, i in zip(expd, inv)]
    return [jnp.dot(p, c, preferred_element_type=jnp.float32).astype(jnp.bfloat16) for p, c in zip(probs, v)]


def second_kernel(seq_len, head_dim, y0_ref, y1_ref, inv_ref, norm_ref, *refs):
    w_refs, p_ref, a_ref, acc, qkv, xs = refs[:3], *refs[3:]
    which, step = pl.program_id(1), pl.program_id(2)
    last = pl.num_programs(2) - 1
    x = normed((pl.program_id(0) == 0) & (which == 0), step, (y0_ref, y1_ref), inv_ref, norm_ref, xs)
    for i, w_ref in enumerate(w_refs):

        @pl.when(which == i)
        def multiply(i=i, w_ref=w_ref):
            depth = w_ref.shape[0]
            base = jnp.where(step == 0, p_ref[0], acc[...])
            out = base + jnp.dot(x, w_ref[...].reshape(depth, -1), preferred_element_type=jnp.float32)
            acc[...] = out
            qkv[i] = out.astype(jnp.bfloat16)

    @pl.when((which == len(w_refs) - 1) & (step == last))
    def heads():
        tokens, width = a_ref.shape
        row = lax.broadcasted_iota(jnp.int32, (seq_len, seq_len), 0)
        col = lax.broadcasted_iota(jnp.int32, (seq_len, seq_len), 1)
        causal = row >= col
        pair = 2 * head_dim

        @pl.loop(0, width // pair)
        def two_heads(n):
            cols = pl.ds(pl.multiple_of(n * pair, pair), pair)
            spans = [(t, h) for h in range(0, pair, head_dim) for t in range(0, tokens, seq_len)]
            parts = [qkv[i, :, cols] for i in range(3)]
            args = [[part[t:t + seq_len, h:h + head_dim] for t, h in spans] for part in parts]
            outs = attend(causal, head_dim ** -0.5, *args)
            for (t, h), out in zip(spans, outs):
                a_ref[t:t + seq_len, pl.ds(pl.multiple_of(n * pair + h, head_dim), head_dim)] = out


def project_first(ys, inv, norm_w, weights):
    rows, width = ys[0].shape
    tokens = inv.shape[0]
    _, heads, head_dim = weights[0].shape
    depth = 512
    steps = width // depth
    cols = GROUP * head_dim
    y_spec = pl.BlockSpec((rows, depth), lambda g, k: (0, jnp.where(g == 0, k, steps - 1)))
    in_specs = [
        y_spec,
        y_spec,
        pl.BlockSpec(inv.shape, lambda g, k: (0, 0)),
        pl.BlockSpec((1, depth), lambda g, k: (0, k)),
    ] + [pl.BlockSpec((depth, GROUP, head_dim), lambda g, k: (k, g, 0))] * 3
    flops = 6 * tokens * width * heads * head_dim
    return pl.pallas_call(
        first_kernel,
        out_shape=jax.ShapeDtypeStruct((3, tokens, heads * head_dim), jnp.float32),
        grid=(heads // GROUP, steps),
        in_specs=in_specs,
        out_specs=pl.BlockSpec((3, tokens, cols), lambda g, k: (0, 0, g)),
        scratch_shapes=[pltpu.VMEM((steps, tokens, depth), jnp.bfloat16)],
        compiler_params=pltpu.CompilerParams(vmem_limit_bytes=57 * 2 ** 20),
        cost_estimate=pl.CostEstimate(flops=flops, bytes_accessed=flops // tokens, transcendentals=0),
        name='first',
    )(*ys, inv, norm_w, *weights)


def project_second(ys, inv, norm_w, weights, partial, seq_len):
    rows, width = ys[0].shape
    tokens = inv.shape[0]
    _, heads, head_dim = weights[0].shape
    depth = 1024
    steps = width // depth
    assert steps == 2
    cols = GROUP * head_dim
    y_spec = pl.BlockSpec((rows, depth), lambda g, i, k: (0, jnp.where((g == 0) & (i == 0), k, steps - 1)))

    def w_spec(own):
        def index(g, i, k):
            at = jnp.maximum(g * steps + jnp.where(i == own, k, jnp.where(i > own, steps - 1, -1)), 0)
            return steps + at % steps, at // steps, 0

        return pl.BlockSpec((depth, GROUP, head_dim), index)

    in_specs = [
        y_spec,
        y_spec,
        pl.BlockSpec(inv.shape, lambda g, i, k: (0, 0)),
        pl.BlockSpec((1, depth), lambda g, i, k: (0, steps + k)),
        *(w_spec(own) for own in range(3)),
        pl.BlockSpec((1, tokens, cols), lambda g, i, k: (i, 0, g)),
    ]
    flops = 6 * tokens * width * heads * head_dim
    return pl.pallas_call(
        functools.partial(second_kernel, seq_len, head_dim),
        out_shape=jax.ShapeDtypeStruct((tokens, heads * head_dim), jnp.bfloat16),
        grid=(heads // GROUP, 3, steps),
        in_specs=in_specs,
        out_specs=pl.BlockSpec((tokens, cols), lambda g, i, k: (0, g)),
        scratch_shapes=[
            pltpu.VMEM((tokens, cols), jnp.float32),
            pltpu.VMEM((3, tokens, cols), jnp.bfloat16),
            pltpu.VMEM((steps, tokens, depth), jnp.bfloat16),
        ],
        compiler_params=pltpu.CompilerParams(vmem_limit_bytes=57 * 2 ** 20),
        cost_estimate=pl.CostEstimate(flops=flops, bytes_accessed=flops // tokens, transcendentals=0),
        name='second',
    )(*ys, inv, norm_w, *weights, partial)


def out_kernel(y_refs_per_half, a_ref, w_ref, *refs):
    o_ref = refs[-1]
    out = jnp.dot(a_ref[...], w_ref[...], preferred_element_type=jnp.float32).astype(jnp.bfloat16).astype(jnp.float32)
    steps = pl.num_programs(0) // HALVES
    rows = refs[0].shape[0]
    for c in range(HALVES):

        @pl.when(pl.program_id(0) // steps == c)
        def store(c=c):
            for m in range(y_refs_per_half):
                wide = refs[c * y_refs_per_half + m][...].astype(jnp.float32)
                span = slice(m * rows, (m + 1) * rows)
                o_ref[span, :] = (wide + out[span]).astype(jnp.bfloat16)


def project_out(attn, w_out, ys):
    tokens, inner = attn.shape
    d_model = w_out.shape[1]
    col = 512
    steps = d_model // HALVES // col
    y_specs = [
        pl.BlockSpec((y.shape[0], col), lambda n, c=c: (0, jnp.clip(n - c * steps, 0, steps - 1)))
        for c in range(HALVES) for y in ys[c]
    ]
    flops = 2 * tokens * inner * d_model
    return pl.pallas_call(
        functools.partial(out_kernel, len(ys[0])),
        out_shape=jax.ShapeDtypeStruct((tokens, d_model), jnp.bfloat16),
        grid=(HALVES * steps,),
        in_specs=[pl.BlockSpec((tokens, inner), lambda n: (0, 0)), pl.BlockSpec((inner, col), lambda n: (0, n))] + y_specs,
        out_specs=pl.BlockSpec((tokens, col), lambda n: (0, n)),
        compiler_params=pltpu.CompilerParams(vmem_limit_bytes=56 * 2 ** 20),
        cost_estimate=pl.CostEstimate(flops=flops, bytes_accessed=flops // tokens, transcendentals=0),
        name='out',
    )(attn, w_out, *ys[0], *ys[1])


def solution(mesh):
    stages = mesh.shape['pp']
    send_next = [(src_row, (src_row + 1) % stages) for src_row in range(stages)]
    swap = [(0, 1), (1, 0)]
    tok_spec = P('pp', 'ep', None, None)
    wt_spec = P('pp', None, None, None)

    def step(expert_out, expert_ids, slot_ids, gate_vals, residual, norm_w, w_query, w_key, w_value, w_out):
        num_micro, seqs_dev, seq_len, d_model = residual.shape
        experts, cap = expert_out.shape[1:3]
        half = cap // 2
        slots = experts * half
        tokens = seqs_dev * seq_len
        me = lax.axis_index('ep').astype(jnp.int32)
        code = jnp.where(slot_ids >= 0, expert_ids * half + slot_ids - me * half, -1)
        theirs = lax.ppermute(jnp.stack([code.astype(jnp.float32), gate_vals]), 'ep', swap)
        flat = (num_micro, tokens, -1)
        first = me * slots
        w_their = gates(theirs[0].astype(jnp.int32).reshape(flat) - first, theirs[1].reshape(flat), slots, norm_w)
        flat_h = residual.reshape(num_micro * tokens, d_model)
        arrived, squares, after = [], 0.0, w_their
        for c in range(HALVES):
            got = []
            for m in range(num_micro):
                part, = mix(expert_out, m, c, 1 - me, w_their, after)
                got.append(lax.ppermute(part, 'ep', swap))
                after = part
            if c == 0:
                w_own = gates(code.reshape(flat) - first, gate_vals.reshape(flat), slots, after)
            ys, sums = [], []
            for m in range(num_micro):
                after, total = mix(expert_out, m, c, me, w_own, after, (flat_h, got[m]))
                sums.append(total[:, 0])
                ys.append(lax.ppermute(after, 'pp', send_next))
            arrived.append(ys)
            squares += jnp.stack(sums)
        squares = lax.ppermute(squares, 'pp', send_next)
        inv_rms = lax.rsqrt(squares.reshape(-1, 1) / d_model + NORM_EPS)
        inv_rms = jnp.broadcast_to(inv_rms, (num_micro * tokens, 128))
        weights = (w_query[0], w_key[0], w_value[0])
        partial = project_first(arrived[0], inv_rms, norm_w, weights)
        out = project_second(arrived[1], inv_rms, norm_w, weights, partial, seq_len)
        result = project_out(out, w_out[0].reshape(-1, d_model), arrived)
        return result.reshape(num_micro, seqs_dev, seq_len, d_model)

    return jax.shard_map(step, mesh=mesh, in_specs=(tok_spec, tok_spec, tok_spec, tok_spec, tok_spec, P('pp', None), wt_spec, wt_spec, wt_spec, wt_spec), out_specs=tok_spec, check_vma=False)
```

```python
import functools

import jax
import jax.numpy as jnp
from jax import lax
from jax.experimental import pallas as pl
from jax.experimental.pallas import tpu as pltpu
from jax.sharding import PartitionSpec as P


NORM_EPS = 1e-6
GROUP = 8
HALVES = 2


def gates_kernel(code_ref, gate_ref, after_ref, w_ref):
    tokens, top_k = code_ref.shape[1:]
    slots = w_ref.shape[2]
    rows, lanes = 64, 512
    for t0 in range(0, tokens, rows):
        code = code_ref[0, t0:t0 + rows, :]
        gate = gate_ref[0, t0:t0 + rows, :]
        for s0 in range(0, slots, lanes):
            lane = lax.broadcasted_iota(jnp.int32, (rows, lanes), 1) + s0
            full = jnp.zeros((rows, lanes), jnp.float32)
            for i in range(top_k):
                full = jnp.where(lane == code[:, i:i + 1], gate[:, i:i + 1], full)
            for part in range(3):
                val = full.astype(jnp.bfloat16)
                w_ref[0, part * tokens + t0:part * tokens + t0 + rows, s0:s0 + lanes] = val
                full = full - val.astype(jnp.float32)


def gates(code, gate, slots, after):
    rows, tokens, top_k = code.shape
    spec = pl.BlockSpec((1, tokens, top_k), lambda m: (m, 0, 0))
    return pl.pallas_call(
        gates_kernel,
        out_shape=jax.ShapeDtypeStruct((rows, 3 * tokens, slots), jnp.bfloat16),
        grid=(rows,),
        in_specs=[spec, spec, pl.BlockSpec(memory_space=pl.ANY)],
        out_specs=pl.BlockSpec((1, 3 * tokens, slots), lambda m: (m, 0, 0)),
        compiler_params=pltpu.CompilerParams(vmem_limit_bytes=16 * 2 ** 20),
        cost_estimate=pl.CostEstimate(flops=rows * tokens * slots * 64, bytes_accessed=6 * rows * tokens * slots, transcendentals=0),
        name='gates',
    )(code, gate, after)


def mix_kernel(has_add, side_ref, w_ref, exp_ref, after_ref, *rest):
    out_ref = rest[2] if has_add else rest[0]
    slots = w_ref.shape[2]
    tokens = w_ref.shape[1] // 3
    exp_rows = exp_ref[0].reshape(slots, exp_ref.shape[3])
    middle = 3 * tokens // 2
    parts = jnp.concatenate([
        jnp.dot(w_ref[0, :middle], exp_rows, preferred_element_type=jnp.float32),
        jnp.dot(w_ref[0, middle:], exp_rows, preferred_element_type=jnp.float32),
    ])
    total = parts[:tokens] + parts[tokens:2 * tokens] + parts[2 * tokens:]
    if has_add:
        total = total + rest[1][...] + rest[0][...].astype(jnp.float32)
    out_ref[...] = total.astype(out_ref.dtype)
    if has_add:
        square_ref = rest[3]

        @pl.when(pl.program_id(0) == 0)
        def clear():
            square_ref[...] = jnp.zeros_like(square_ref)

        wide = total.astype(jnp.bfloat16).astype(jnp.float32)
        square_ref[...] += jnp.sum(wide * wide, axis=1, keepdims=True)


def mix(expert_out, row, piece, side, w, after, add=None):
    _, rows3, slots = w.shape
    tokens = rows3 // 3
    _, experts, cap, d_model = expert_out.shape
    width = d_model // HALVES
    col = 512
    steps = width // col
    in_specs = [
        pl.BlockSpec((1, rows3, slots), lambda c, s: (row, 0, 0)),
        pl.BlockSpec((1, experts, cap // 2, col), lambda c, s: (row, 0, s[0], piece * steps + c)),
        pl.BlockSpec(memory_space=pl.ANY),
    ]
    args = [w, expert_out, after]
    if add is not None:
        in_specs += [
            pl.BlockSpec((tokens, col), lambda c, s: (row, piece * steps + c)),
            pl.BlockSpec((tokens, col), lambda c, s: (0, c)),
        ]
        args += list(add)
    out_shape = [jax.ShapeDtypeStruct((tokens, width), jnp.float32 if add is None else jnp.bfloat16)]
    out_specs = [pl.BlockSpec((tokens, col), lambda c, s: (0, c))]
    if add is not None:
        out_shape.append(jax.ShapeDtypeStruct((tokens, 128), jnp.float32))
        out_specs.append(pl.BlockSpec((tokens, 128), lambda c, s: (0, 0)))
    return pl.pallas_call(
        functools.partial(mix_kernel, add is not None),
        out_shape=out_shape,
        grid_spec=pltpu.PrefetchScalarGridSpec(
            num_scalar_prefetch=1,
            grid=(steps,),
            in_specs=in_specs,
            out_specs=out_specs,
        ),
        compiler_params=pltpu.CompilerParams(vmem_limit_bytes=16 * 2 ** 20),
        cost_estimate=pl.CostEstimate(flops=2 * rows3 * slots * width, bytes_accessed=2 * slots * width, transcendentals=0),
    )(side.reshape(1), *args)


def normed(first_step, y_refs, inv_ref, norm_ref, xs):
    @pl.when(first_step)
    def make():
        rows = y_refs[0].shape[0]
        for m, y_ref in enumerate(y_refs):

            @pl.loop(0, rows // 32)
            def block(n, m=m, y_ref=y_ref):
                near = pl.ds(pl.multiple_of(n * 32, 32), 32)
                span = pl.ds(pl.multiple_of(m * rows + n * 32, 32), 32)
                wide = y_ref[near, :].astype(jnp.float32)
                xs[span, :] = (wide * inv_ref[span, :1] * norm_ref[...]).astype(jnp.bfloat16)


def matmul(xs, w_ref):
    return jnp.dot(xs[...], w_ref[...].reshape(w_ref.shape[0], -1), preferred_element_type=jnp.float32)


def first_kernel(y0_ref, y1_ref, inv_ref, norm_ref, *refs):
    which = pl.program_id(1)
    w_refs, o_ref, xs = refs[:3], *refs[3:]
    normed((pl.program_id(0) == 0) & (which == 0), (y0_ref, y1_ref), inv_ref, norm_ref, xs)
    for i, w_ref in enumerate(w_refs):

        @pl.when(which == i)
        def multiply(w_ref=w_ref):
            o_ref[0] = matmul(xs, w_ref)


def attend(causal, scale, q, k, v):
    dims = (((1,), (1,)), ((), ()))
    scores = [lax.dot_general(a, b, dims, preferred_element_type=jnp.float32) for a, b in zip(q, k)]
    scores = [jnp.where(causal, s * scale, -jnp.inf) for s in scores]
    tops = [jnp.max(s, axis=1, keepdims=True) for s in scores]
    expd = [jnp.exp(s - t) for s, t in zip(scores, tops)]
    inv = [1.0 / jnp.sum(e, axis=1, keepdims=True) for e in expd]
    probs = [(e * i).astype(jnp.bfloat16) for e, i in zip(expd, inv)]
    return [jnp.dot(p, c, preferred_element_type=jnp.float32).astype(jnp.bfloat16) for p, c in zip(probs, v)]


def second_kernel(seq_len, head_dim, y0_ref, y1_ref, inv_ref, norm_ref, *refs):
    w_refs, p_ref, a_ref, qkv, xs = refs[:3], *refs[3:]
    group, which = pl.program_id(0), pl.program_id(1)
    groups = pl.num_programs(0) - 1
    tokens, width = a_ref.shape
    heads = width // head_dim
    normed((group == 0) & (which == 0), (y0_ref, y1_ref), inv_ref, norm_ref, xs)
    now, before = lax.rem(group, 2), lax.rem(group + 1, 2)
    bounds = [-(-heads * i // 3) for i in range(4)]

    def attend_some(i):
        row = lax.broadcasted_iota(jnp.int32, (seq_len, seq_len), 0)
        col = lax.broadcasted_iota(jnp.int32, (seq_len, seq_len), 1)
        for h in range(bounds[i] * head_dim, bounds[i + 1] * head_dim, head_dim):
            spans = range(0, tokens, seq_len)
            args = [[qkv[before, j, t:t + seq_len, h:h + head_dim] for t in spans] for j in range(3)]
            for t, out in zip(spans, attend(row >= col, head_dim ** -0.5, *args)):
                a_ref[t:t + seq_len, h:h + head_dim] = out

    for i, w_ref in enumerate(w_refs):

        @pl.when((which == i) & (group < groups))
        def both(i=i, w_ref=w_ref):
            qkv[now, i] = (p_ref[0] + matmul(xs, w_ref)).astype(jnp.bfloat16)
            attend_some(i)

        @pl.when((which == i) & (group == groups))
        def rest(i=i):
            attend_some(i)


def project(piece, ys, inv, norm_w, weights, partial, seq_len):
    rows, width = ys[0].shape
    tokens = inv.shape[0]
    _, heads, head_dim = weights[0].shape
    cols = GROUP * head_dim
    groups = heads // GROUP

    def w_spec(own):
        def index(g, i):
            return piece, jnp.clip(jnp.where(i >= own, g, g - 1), 0, groups - 1), 0

        return pl.BlockSpec((width, GROUP, head_dim), index)

    whole = pl.BlockSpec((rows, width), lambda g, i: (0, 0))
    in_specs = [
        whole,
        whole,
        pl.BlockSpec(inv.shape, lambda g, i: (0, 0)),
        pl.BlockSpec((1, width), lambda g, i: (0, piece)),
        *(w_spec(own) for own in range(3)),
    ]
    xs = pltpu.VMEM((tokens, width), jnp.bfloat16)
    flops = 6 * tokens * width * heads * head_dim
    settings = dict(
        compiler_params=pltpu.CompilerParams(vmem_limit_bytes=57 * 2 ** 20),
        cost_estimate=pl.CostEstimate(flops=flops, bytes_accessed=flops // tokens, transcendentals=0),
    )
    args = (*ys, inv, norm_w, *weights)
    if partial is None:
        return pl.pallas_call(
            first_kernel,
            out_shape=jax.ShapeDtypeStruct((3, tokens, heads * head_dim), jnp.float32),
            grid=(groups, 3),
            in_specs=in_specs,
            out_specs=pl.BlockSpec((1, tokens, cols), lambda g, i: (i, 0, g)),
            scratch_shapes=[xs],
            name='first',
            **settings,
        )(*args)
    return pl.pallas_call(
        functools.partial(second_kernel, seq_len, head_dim),
        out_shape=jax.ShapeDtypeStruct((tokens, heads * head_dim), jnp.bfloat16),
        grid=(groups + 1, 3),
        in_specs=in_specs + [pl.BlockSpec((1, tokens, cols), lambda g, i: (jnp.where(g < groups, i, 2), 0, jnp.minimum(g, groups - 1)))],
        out_specs=pl.BlockSpec((tokens, cols), lambda g, i: (0, jnp.maximum(g - 1, 0))),
        scratch_shapes=[pltpu.VMEM((2, 3, tokens, cols), jnp.bfloat16), xs],
        name='second',
        **settings,
    )(*args, partial)


def out_kernel(y_refs_per_half, a_ref, w_ref, *refs):
    o_ref = refs[-1]
    out = jnp.dot(a_ref[...], w_ref[...], preferred_element_type=jnp.float32).astype(jnp.bfloat16).astype(jnp.float32)
    steps = pl.num_programs(0) // HALVES
    rows = refs[0].shape[0]
    for c in range(HALVES):

        @pl.when(pl.program_id(0) // steps == c)
        def store(c=c):
            for m in range(y_refs_per_half):
                wide = refs[c * y_refs_per_half + m][...].astype(jnp.float32)
                span = slice(m * rows, (m + 1) * rows)
                o_ref[span, :] = (wide + out[span]).astype(jnp.bfloat16)


def project_out(attn, w_out, ys):
    tokens, inner = attn.shape
    d_model = w_out.shape[1]
    col = 512
    steps = d_model // HALVES // col
    y_specs = [
        pl.BlockSpec((y.shape[0], col), lambda n, c=c: (0, jnp.clip(n - c * steps, 0, steps - 1)))
        for c in range(HALVES) for y in ys[c]
    ]
    flops = 2 * tokens * inner * d_model
    return pl.pallas_call(
        functools.partial(out_kernel, len(ys[0])),
        out_shape=jax.ShapeDtypeStruct((tokens, d_model), jnp.bfloat16),
        grid=(HALVES * steps,),
        in_specs=[pl.BlockSpec((tokens, inner), lambda n: (0, 0)), pl.BlockSpec((inner, col), lambda n: (0, n))] + y_specs,
        out_specs=pl.BlockSpec((tokens, col), lambda n: (0, n)),
        compiler_params=pltpu.CompilerParams(vmem_limit_bytes=56 * 2 ** 20),
        cost_estimate=pl.CostEstimate(flops=flops, bytes_accessed=flops // tokens, transcendentals=0),
        name='out',
    )(attn, w_out, *ys[0], *ys[1])


def solution(mesh):
    stages = mesh.shape['pp']
    send_next = [(src_row, (src_row + 1) % stages) for src_row in range(stages)]
    swap = [(0, 1), (1, 0)]
    tok_spec = P('pp', 'ep', None, None)
    wt_spec = P('pp', None, None, None)

    def step(expert_out, expert_ids, slot_ids, gate_vals, residual, norm_w, w_query, w_key, w_value, w_out):
        num_micro, seqs_dev, seq_len, d_model = residual.shape
        experts, cap = expert_out.shape[1:3]
        half = cap // 2
        slots = experts * half
        tokens = seqs_dev * seq_len
        me = lax.axis_index('ep').astype(jnp.int32)
        code = jnp.where(slot_ids >= 0, expert_ids * half + slot_ids - me * half, -1)
        theirs = lax.ppermute(jnp.stack([code.astype(jnp.float32), gate_vals]), 'ep', swap)
        flat = (num_micro, tokens, -1)
        first = me * slots
        w_their = gates(theirs[0].astype(jnp.int32).reshape(flat) - first, theirs[1].reshape(flat), slots, norm_w)
        flat_h = residual.reshape(num_micro * tokens, d_model)
        arrived, squares, after = [], 0.0, w_their
        for c in range(HALVES):
            got = []
            for m in range(num_micro):
                part, = mix(expert_out, m, c, 1 - me, w_their, after)
                got.append(lax.ppermute(part, 'ep', swap))
                after = part
            if c == 0:
                w_own = gates(code.reshape(flat) - first, gate_vals.reshape(flat), slots, after)
            ys, sums = [], []
            for m in range(num_micro):
                after, total = mix(expert_out, m, c, me, w_own, after, (flat_h, got[m]))
                sums.append(total[:, 0])
                ys.append(lax.ppermute(after, 'pp', send_next))
            arrived.append(ys)
            squares += jnp.stack(sums)
        squares = lax.ppermute(squares, 'pp', send_next)
        inv_rms = lax.rsqrt(squares.reshape(-1, 1) / d_model + NORM_EPS)
        inv_rms = jnp.broadcast_to(inv_rms, (num_micro * tokens, 128))
        weights = (w_query[0], w_key[0], w_value[0])
        partial = None
        for c in range(HALVES):
            partial = project(c, arrived[c], inv_rms, norm_w, weights, partial, seq_len)
        result = project_out(partial, w_out[0].reshape(-1, d_model), arrived)
        return result.reshape(num_micro, seqs_dev, seq_len, d_model)

    return jax.shard_map(step, mesh=mesh, in_specs=(tok_spec, tok_spec, tok_spec, tok_spec, tok_spec, P('pp', None), wt_spec, wt_spec, wt_spec, wt_spec), out_specs=tok_spec, check_vma=False)
```

```python
import functools

import jax
import jax.numpy as jnp
from jax import lax
from jax.experimental import pallas as pl
from jax.experimental.pallas import tpu as pltpu
from jax.sharding import PartitionSpec as P


NORM_EPS = 1e-6
GROUP = 8
HALVES = 2


def gates_kernel(code_ref, gate_ref, after_ref, w_ref):
    tokens, top_k = code_ref.shape[1:]
    slots = w_ref.shape[2]
    rows, lanes = 64, 512
    for t0 in range(0, tokens, rows):
        code = code_ref[0, t0:t0 + rows, :]
        gate = gate_ref[0, t0:t0 + rows, :]
        for s0 in range(0, slots, lanes):
            lane = lax.broadcasted_iota(jnp.int32, (rows, lanes), 1) + s0
            full = jnp.zeros((rows, lanes), jnp.float32)
            for i in range(top_k):
                full = jnp.where(lane == code[:, i:i + 1], gate[:, i:i + 1], full)
            for part in range(3):
                val = full.astype(jnp.bfloat16)
                w_ref[0, part * tokens + t0:part * tokens + t0 + rows, s0:s0 + lanes] = val
                full = full - val.astype(jnp.float32)


def gates(code, gate, slots, after):
    rows, tokens, top_k = code.shape
    spec = pl.BlockSpec((1, tokens, top_k), lambda m: (m, 0, 0))
    return pl.pallas_call(
        gates_kernel,
        out_shape=jax.ShapeDtypeStruct((rows, 3 * tokens, slots), jnp.bfloat16),
        grid=(rows,),
        in_specs=[spec, spec, pl.BlockSpec(memory_space=pl.ANY)],
        out_specs=pl.BlockSpec((1, 3 * tokens, slots), lambda m: (m, 0, 0)),
        compiler_params=pltpu.CompilerParams(vmem_limit_bytes=16 * 2 ** 20),
        cost_estimate=pl.CostEstimate(flops=rows * tokens * slots * 64, bytes_accessed=6 * rows * tokens * slots, transcendentals=0),
        name='gates',
    )(code, gate, after)


def mix_kernel(has_add, side_ref, w_ref, exp_ref, after_ref, *rest):
    out_ref = rest[2] if has_add else rest[0]
    slots = w_ref.shape[2]
    tokens = w_ref.shape[1] // 3
    exp_rows = exp_ref[0].reshape(slots, exp_ref.shape[3])
    middle = 3 * tokens // 2
    parts = jnp.concatenate([
        jnp.dot(w_ref[0, :middle], exp_rows, preferred_element_type=jnp.float32),
        jnp.dot(w_ref[0, middle:], exp_rows, preferred_element_type=jnp.float32),
    ])
    total = parts[:tokens] + parts[tokens:2 * tokens] + parts[2 * tokens:]
    if has_add:
        total = total + rest[1][...] + rest[0][...].astype(jnp.float32)
    out_ref[...] = total.astype(out_ref.dtype)
    if has_add:
        square_ref = rest[3]

        @pl.when(pl.program_id(0) == 0)
        def clear():
            square_ref[...] = jnp.zeros_like(square_ref)

        wide = total.astype(jnp.bfloat16).astype(jnp.float32)
        square_ref[...] += jnp.sum(wide * wide, axis=1, keepdims=True)


def mix(expert_out, row, piece, side, w, after, add=None):
    _, rows3, slots = w.shape
    tokens = rows3 // 3
    _, experts, cap, d_model = expert_out.shape
    width = d_model // HALVES
    col = 512
    steps = width // col
    in_specs = [
        pl.BlockSpec((1, rows3, slots), lambda c, s: (row, 0, 0)),
        pl.BlockSpec((1, experts, cap // 2, col), lambda c, s: (row, 0, s[0], piece * steps + c)),
        pl.BlockSpec(memory_space=pl.ANY),
    ]
    args = [w, expert_out, after]
    if add is not None:
        in_specs += [
            pl.BlockSpec((tokens, col), lambda c, s: (row, piece * steps + c)),
            pl.BlockSpec((tokens, col), lambda c, s: (0, c)),
        ]
        args += list(add)
    out_shape = [jax.ShapeDtypeStruct((tokens, width), jnp.float32 if add is None else jnp.bfloat16)]
    out_specs = [pl.BlockSpec((tokens, col), lambda c, s: (0, c))]
    if add is not None:
        out_shape.append(jax.ShapeDtypeStruct((tokens, 128), jnp.float32))
        out_specs.append(pl.BlockSpec((tokens, 128), lambda c, s: (0, 0)))
    return pl.pallas_call(
        functools.partial(mix_kernel, add is not None),
        out_shape=out_shape,
        grid_spec=pltpu.PrefetchScalarGridSpec(
            num_scalar_prefetch=1,
            grid=(steps,),
            in_specs=in_specs,
            out_specs=out_specs,
        ),
        compiler_params=pltpu.CompilerParams(vmem_limit_bytes=16 * 2 ** 20),
        cost_estimate=pl.CostEstimate(flops=2 * rows3 * slots * width, bytes_accessed=2 * slots * width, transcendentals=0),
    )(side.reshape(1), *args)


def normed(first_step, y_refs, inv_ref, norm_ref, xs):
    @pl.when(first_step)
    def make():
        rows = y_refs[0].shape[0]
        for m, y_ref in enumerate(y_refs):

            @pl.loop(0, rows // 32)
            def block(n, m=m, y_ref=y_ref):
                near = pl.ds(pl.multiple_of(n * 32, 32), 32)
                span = pl.ds(pl.multiple_of(m * rows + n * 32, 32), 32)
                wide = y_ref[near, :].astype(jnp.float32)
                xs[span, :] = (wide * inv_ref[span, :1] * norm_ref[...]).astype(jnp.bfloat16)


def first_kernel(y0_ref, y1_ref, inv_ref, norm_ref, *refs):
    w_refs, o_ref, xs = refs[:3], *refs[3:]
    normed(pl.program_id(0) == 0, (y0_ref, y1_ref), inv_ref, norm_ref, xs)
    for i, w_ref in enumerate(w_refs):
        o_ref[i] = jnp.dot(xs[...], w_ref[...].reshape(xs.shape[1], -1), preferred_element_type=jnp.float32)


def scores_of(causal, scale, q, k):
    dims = (((1,), (1,)), ((), ()))
    scores = [lax.dot_general(a, b, dims, preferred_element_type=jnp.float32) for a, b in zip(q, k)]
    return [jnp.where(causal, s * scale, -jnp.inf) for s in scores]


def softmax_of(scores):
    tops = [jnp.max(s, axis=1, keepdims=True) for s in scores]
    expd = [jnp.exp(s - t) for s, t in zip(scores, tops)]
    inv = [1.0 / jnp.sum(e, axis=1, keepdims=True) for e in expd]
    return [(e * i).astype(jnp.bfloat16) for e, i in zip(expd, inv)]


def second_kernel(seq_len, head_dim, y0_ref, y1_ref, inv_ref, norm_ref, *refs):
    w_refs, p_ref, a_ref, xs, qkv = refs[:3], *refs[3:]
    group = pl.program_id(0)
    groups = pl.num_programs(0) - 1
    tokens, cols = a_ref.shape
    now, before = lax.rem(group, 2), lax.rem(group + 1, 2)
    normed(group == 0, (y0_ref, y1_ref), inv_ref, norm_ref, xs)
    spans = range(0, tokens, seq_len)

    def heads_at(j, h):
        return [qkv[before, j, t:t + seq_len, h:h + head_dim] for t in spans]

    def score(h):
        row = lax.broadcasted_iota(jnp.int32, (seq_len, seq_len), 0)
        col = lax.broadcasted_iota(jnp.int32, (seq_len, seq_len), 1)
        return scores_of(row >= col, head_dim ** -0.5, heads_at(0, h), heads_at(1, h))

    def mix_values(h, scores):
        for t, prob, value in zip(spans, softmax_of(scores), heads_at(2, h)):
            out = jnp.dot(prob, value, preferred_element_type=jnp.float32)
            a_ref[t:t + seq_len, h:h + head_dim] = out.astype(jnp.bfloat16)

    @pl.when(group < groups)
    def both():
        width = 512
        chunks = 3 * cols // width
        heads = cols // head_dim
        for i in range(3):
            w = w_refs[i][...].reshape(xs.shape[1], -1)
            for n in range(0, cols, width):
                at = (i * cols + n) // width
                part = [h * head_dim for h in range(heads * at // chunks, heads * (at + 1) // chunks)]
                scores = [score(h) for h in part]
                out = jnp.dot(xs[...], w[:, n:n + width], preferred_element_type=jnp.float32)
                qkv[now, i, :, n:n + width] = (p_ref[i, :, n:n + width] + out).astype(jnp.bfloat16)
                for h, score_h in zip(part, scores):
                    mix_values(h, score_h)

    @pl.when(group == groups)
    def rest():
        for h in range(0, cols, head_dim):
            mix_values(h, score(h))


def project(piece, ys, inv, norm_w, weights, partial, seq_len):
    rows, width = ys[0].shape
    tokens = inv.shape[0]
    _, heads, head_dim = weights[0].shape
    cols = GROUP * head_dim
    groups = heads // GROUP
    w_spec = pl.BlockSpec((width, GROUP, head_dim), lambda g: (piece, jnp.minimum(g, groups - 1), 0))
    o_spec = pl.BlockSpec((3, tokens, cols), lambda g: (0, 0, jnp.minimum(g, groups - 1)))
    whole = pl.BlockSpec((rows, width), lambda g: (0, 0))
    in_specs = [
        whole,
        whole,
        pl.BlockSpec(inv.shape, lambda g: (0, 0)),
        pl.BlockSpec((1, width), lambda g: (0, piece)),
        w_spec,
        w_spec,
        w_spec,
    ]
    scratch = [pltpu.VMEM((tokens, width), jnp.bfloat16)]
    flops = 6 * tokens * width * heads * head_dim
    settings = dict(
        compiler_params=pltpu.CompilerParams(vmem_limit_bytes=(52 if partial is None else 57) * 2 ** 20),
        cost_estimate=pl.CostEstimate(flops=flops, bytes_accessed=flops // tokens, transcendentals=0),
    )
    args = (*ys, inv, norm_w, *weights)
    if partial is None:
        return pl.pallas_call(
            first_kernel,
            out_shape=jax.ShapeDtypeStruct((3, tokens, heads * head_dim), jnp.float32),
            grid=(groups,),
            in_specs=in_specs,
            out_specs=o_spec,
            scratch_shapes=scratch,
            name='first',
            **settings,
        )(*args)
    return pl.pallas_call(
        functools.partial(second_kernel, seq_len, head_dim),
        out_shape=jax.ShapeDtypeStruct((tokens, heads * head_dim), jnp.bfloat16),
        grid=(groups + 1,),
        in_specs=in_specs + [o_spec],
        out_specs=pl.BlockSpec((tokens, cols), lambda g: (0, jnp.maximum(g - 1, 0))),
        scratch_shapes=scratch + [
            pltpu.VMEM((2, 3, tokens, cols), jnp.bfloat16),
        ],
        name='second',
        **settings,
    )(*args, partial)


def out_kernel(y_refs_per_half, a_ref, w_ref, *refs):
    o_ref = refs[-1]
    out = jnp.dot(a_ref[...], w_ref[...], preferred_element_type=jnp.float32).astype(jnp.bfloat16).astype(jnp.float32)
    steps = pl.num_programs(0) // HALVES
    rows = refs[0].shape[0]
    for c in range(HALVES):

        @pl.when(pl.program_id(0) // steps == c)
        def store(c=c):
            for m in range(y_refs_per_half):
                wide = refs[c * y_refs_per_half + m][...].astype(jnp.float32)
                span = slice(m * rows, (m + 1) * rows)
                o_ref[span, :] = (wide + out[span]).astype(jnp.bfloat16)


def project_out(attn, w_out, ys):
    tokens, inner = attn.shape
    d_model = w_out.shape[1]
    col = 512
    steps = d_model // HALVES // col
    y_specs = [
        pl.BlockSpec((y.shape[0], col), lambda n, c=c: (0, jnp.clip(n - c * steps, 0, steps - 1)))
        for c in range(HALVES) for y in ys[c]
    ]
    flops = 2 * tokens * inner * d_model
    return pl.pallas_call(
        functools.partial(out_kernel, len(ys[0])),
        out_shape=jax.ShapeDtypeStruct((tokens, d_model), jnp.bfloat16),
        grid=(HALVES * steps,),
        in_specs=[pl.BlockSpec((tokens, inner), lambda n: (0, 0)), pl.BlockSpec((inner, col), lambda n: (0, n))] + y_specs,
        out_specs=pl.BlockSpec((tokens, col), lambda n: (0, n)),
        compiler_params=pltpu.CompilerParams(vmem_limit_bytes=48 * 2 ** 20),
        cost_estimate=pl.CostEstimate(flops=flops, bytes_accessed=flops // tokens, transcendentals=0),
        name='out',
    )(attn, w_out, *ys[0], *ys[1])


def solution(mesh):
    stages = mesh.shape['pp']
    send_next = [(src_row, (src_row + 1) % stages) for src_row in range(stages)]
    swap = [(0, 1), (1, 0)]
    tok_spec = P('pp', 'ep', None, None)
    wt_spec = P('pp', None, None, None)

    def step(expert_out, expert_ids, slot_ids, gate_vals, residual, norm_w, w_query, w_key, w_value, w_out):
        num_micro, seqs_dev, seq_len, d_model = residual.shape
        experts, cap = expert_out.shape[1:3]
        half = cap // 2
        slots = experts * half
        tokens = seqs_dev * seq_len
        me = lax.axis_index('ep').astype(jnp.int32)
        code = jnp.where(slot_ids >= 0, expert_ids * half + slot_ids - me * half, -1)
        theirs = lax.ppermute(jnp.stack([code.astype(jnp.float32), gate_vals]), 'ep', swap)
        flat = (num_micro, tokens, -1)
        first = me * slots
        w_their = gates(theirs[0].astype(jnp.int32).reshape(flat) - first, theirs[1].reshape(flat), slots, norm_w)
        flat_h = residual.reshape(num_micro * tokens, d_model)
        got, arrived, sums, after = {}, {}, {}, w_their

        def their(c, m):
            part, = mix(expert_out, m, c, 1 - me, w_their, after)
            got[c, m] = lax.ppermute(part, 'ep', swap)
            return part

        def own(c, m):
            y, total = mix(expert_out, m, c, me, w_own, after, (flat_h, got[c, m]))
            sums[c, m] = total[:, 0]
            arrived[c, m] = lax.ppermute(y, 'pp', send_next)
            return y

        after = their(0, 0)
        w_own = gates(code.reshape(flat) - first, gate_vals.reshape(flat), slots, after)
        for side, c, m in ((own, 0, 0), (their, 0, 1), (their, 1, 0), (own, 0, 1), (their, 1, 1), (own, 1, 0), (own, 1, 1)):
            after = side(c, m)
        arrived = [[arrived[c, m] for m in range(num_micro)] for c in range(HALVES)]
        squares = jnp.stack([sums[0, m] + sums[1, m] for m in range(num_micro)])
        squares = lax.ppermute(squares, 'pp', send_next)
        inv_rms = lax.rsqrt(squares.reshape(-1, 1) / d_model + NORM_EPS)
        inv_rms = jnp.broadcast_to(inv_rms, (num_micro * tokens, 128))
        weights = (w_query[0], w_key[0], w_value[0])
        partial = None
        for c in range(HALVES):
            partial = project(c, arrived[c], inv_rms, norm_w, weights, partial, seq_len)
        result = project_out(partial, w_out[0].reshape(-1, d_model), arrived)
        return result.reshape(num_micro, seqs_dev, seq_len, d_model)

    return jax.shard_map(step, mesh=mesh, in_specs=(tok_spec, tok_spec, tok_spec, tok_spec, tok_spec, P('pp', None), wt_spec, wt_spec, wt_spec, wt_spec), out_specs=tok_spec, check_vma=False)
```
